128 devices in a mesh: gx: 4 (over y), gy: 4 (over x), gz: 8 (over z, core).
Axes of the slice: x: 4, y: 4, z: 4, core: 2. Of those that a mesh axis runs over, the one named last changes fastest.
Arguments:
- queries: bfloat16 [65536, 1024], P(('gx', 'gy', 'gz')), may hold values from -6 to 6
- keys: bfloat16 [65536, 1024], P(('gx', 'gy', 'gz')), may hold values from -6 to 6
- values: bfloat16 [65536, 1024], P(('gx', 'gy', 'gz')), may hold values from -6 to 6
- out_grad: bfloat16 [65536, 1024], P(('gx', 'gy', 'gz')), may hold values from -0.0234375 to 0.0234375
- log_decay: float32 [4, 65536], P(None, ('gx', 'gy', 'gz')), may hold values from -0.8 to 0, as said below
- saved_states: bfloat16 [128, 4, 256, 256], P(('gx', 'gy', 'gz')), may hold values from -67.5 to 67.5
Outputs:
- query_grad: bfloat16 [65536, 1024], P(('gx', 'gy', 'gz'))
- key_grad: bfloat16 [65536, 1024], P(('gx', 'gy', 'gz'))
- value_grad: bfloat16 [65536, 1024], P(('gx', 'gy', 'gz'))
The draws below stay inside these ranges and needn't reach their ends.
Inputs may be any that keep to these rules, and one draw needn't show every extreme that they name: `log_decay`: every entry is negative.
All inputs are finite; a program needn't handle non-finite values.
Results may differ from the reference program's by a relative error of at most 0.0056.
Values sent between devices are 32-bit elements; how exact they have to be, the bound alone decides.
A program may use at most 512 MiB of HBM per device.

```python
import math
import jax
import jax.numpy as jnp
from jax import lax

HEAD_GROUP = 4
HEAD_DIM = 256
WIDTH = 1024
TOK_DEV = 512
TOKEN_POSITIONS = 65536
BLOCKS = 128


def draw_log_decay(key, part):
    random_subkeys = jax.random.split(jax.random.fold_in(key, 17), 7)
    head_rank = jax.random.permutation(random_subkeys[0], HEAD_GROUP)
    fast_count = max(1, HEAD_GROUP // 2)
    fast_heads = (head_rank < fast_count)[:, None]
    slow_share = jax.random.uniform(random_subkeys[1], (HEAD_GROUP, 1), jnp.float32, 0.2, 1.0)
    slow_rate = slow_share * (0.25 * math.log(10.0)) / TOKEN_POSITIONS
    fast_rate = jax.random.uniform(random_subkeys[2], (HEAD_GROUP, 1), jnp.float32, 1.0 / 50.0, 1.0 / 30.0)
    baseline_decay_rate = jnp.where(fast_heads, fast_rate, slow_rate)
    block_multiplier = jnp.exp(jax.random.uniform(random_subkeys[3], (HEAD_GROUP, TOKEN_POSITIONS // TOK_DEV), jnp.float32, -math.log(2.0), math.log(2.0)))
    block_multiplier = jnp.repeat(block_multiplier, TOK_DEV, axis=1)
    jaggedness = jax.random.uniform(random_subkeys[4], (HEAD_GROUP, TOKEN_POSITIONS), jnp.float32, 0.5, 1.5)
    spike_positions = jax.random.randint(random_subkeys[5], (2,), 0, TOKEN_POSITIONS)
    chosen_positions = jnp.arange(TOKEN_POSITIONS, dtype=jnp.int32)
    spike_mask = jnp.any(chosen_positions[None, :] == spike_positions[:, None], axis=0)
    spike_length = jnp.log(jax.random.uniform(random_subkeys[6], (HEAD_GROUP, 1), jnp.float32, 0.5, 0.8))
    final_output = -baseline_decay_rate * block_multiplier * jaggedness + jnp.where(spike_mask[None, :], spike_length, 0.0)
    return final_output.astype(jnp.float32)


def block_scale(own_key, shape, cuts, smallest, high):
    level = 1.0
    for axis_at, shards_of in cuts:
        steps = jax.random.uniform(jax.random.fold_in(jax.random.fold_in(own_key, 6), axis_at), (shards_of,), jnp.float32, smallest / len(cuts), high / len(cuts))
        level = level * jnp.repeat(jnp.exp(steps), shape[axis_at] // shards_of).reshape((-1,) + (1,) * (len(shape) - 1 - axis_at))
    return level


def normal_values(own_key, extent, scale, limit, shards=(), held_as=jnp.bfloat16):
    values = scale * jax.random.normal(own_key, extent, jnp.float32)
    if shards:
        values = values * block_scale(own_key, extent, shards, -0.22, 0.18)
    return jnp.clip(values, -limit, limit).astype(held_as)


def setup_inputs(seed: int = 0) -> dict:
    splits = jax.random.split(jax.random.key(seed), 7)
    return {
        "queries": normal_values(splits[0], (TOKEN_POSITIONS, WIDTH), 1.0, 6.0, ((0, 128),)),
        "keys": normal_values(splits[1], (TOKEN_POSITIONS, WIDTH), 1.0, 6.0, ((0, 128),)),
        "values": normal_values(splits[2], (TOKEN_POSITIONS, WIDTH), 1.0, 6.0, ((0, 128),)),
        "out_grad": normal_values(splits[3], (TOKEN_POSITIONS, WIDTH), (TOKEN_POSITIONS ** -0.5), 0.0234375, ((0, 128),)),
        "log_decay": draw_log_decay(jax.random.fold_in(splits[6], 71), 0),
        "saved_states": normal_values(splits[5], (BLOCKS, HEAD_GROUP, HEAD_DIM, HEAD_DIM), (0.5 * TOK_DEV ** 0.5), 67.5, ((0, 128),)),
    }


def reference(queries, keys, values, out_grad, log_decay, saved_states):
    count_blocks = TOKEN_POSITIONS // TOK_DEV
    score_scale = HEAD_DIM ** -0.5

    def blocked(array):
        return array.reshape(count_blocks, TOK_DEV, HEAD_GROUP, HEAD_DIM)

    decay_blocks = log_decay.reshape(HEAD_GROUP, count_blocks, TOK_DEV).transpose(1, 0, 2)
    inputs = (blocked(queries), blocked(keys), blocked(values), blocked(out_grad), decay_blocks, saved_states)
    zero_state = jnp.zeros((HEAD_GROUP, HEAD_DIM, HEAD_DIM), jnp.float32)
    positions = jnp.arange(TOK_DEV, dtype=jnp.int32)
    causal = positions[:, None] >= positions[None, :]

    def backward_step(carry, block_in):
        query_heads, key_heads, value_heads, grad_heads, decay_rows, state_in = block_in
        query_f = query_heads.astype(jnp.float32)
        key_f = key_heads.astype(jnp.float32)
        value_f = value_heads.astype(jnp.float32)
        grad_f = grad_heads.astype(jnp.float32)
        cumulative = jnp.cumsum(decay_rows, axis=1)
        block_end = cumulative[:, -1:]
        to_end = jnp.exp(block_end - cumulative)
        from_start = jnp.exp(cumulative)
        log_gaps = cumulative[:, :, None] - cumulative[:, None, :]
        weight = jnp.where(causal[None], jnp.exp(jnp.minimum(log_gaps, 0.0)), 0.0)
        probs = (jnp.einsum('thd,shd->hts', query_f, key_f) * score_scale * weight).astype(jnp.bfloat16)
        grad_scores = (jnp.einsum('thd,shd->hts', grad_f, value_f) * score_scale * weight).astype(jnp.bfloat16)
        query_decayed = (query_f * (score_scale * from_start).T[:, :, None]).astype(jnp.bfloat16)
        local_grad = jnp.einsum('thi,thj->hij', query_decayed.astype(jnp.float32), grad_f)
        grad_in = carry.astype(jnp.bfloat16).astype(jnp.float32)
        state_f = state_in.astype(jnp.float32)
        probs_f = probs.astype(jnp.float32)
        grad_scores_f = grad_scores.astype(jnp.float32)
        query_grad = jnp.einsum('hts,shd->thd', grad_scores_f, key_f)
        query_grad = query_grad + jnp.einsum('thj,hij->thi', grad_f, state_f) * (score_scale * from_start).T[:, :, None]
        key_grad = jnp.einsum('hts,thd->shd', grad_scores_f, query_f)
        key_grad = key_grad + jnp.einsum('thj,hij->thi', value_f, grad_in) * to_end.T[:, :, None]
        value_grad = jnp.einsum('hts,thd->shd', probs_f, grad_f)
        value_grad = value_grad + jnp.einsum('thi,hij->thj', key_f, grad_in) * to_end.T[:, :, None]
        new_carry = jnp.exp(block_end[:, 0])[:, None, None] * carry + local_grad
        return new_carry, (query_grad.astype(jnp.bfloat16), key_grad.astype(jnp.bfloat16), value_grad.astype(jnp.bfloat16))

    last_carry, grads = lax.scan(backward_step, zero_state, inputs, reverse=True)
    query_grad = grads[0].reshape(TOKEN_POSITIONS, WIDTH)
    key_grad = grads[1].reshape(TOKEN_POSITIONS, WIDTH)
    value_grad = grads[2].reshape(TOKEN_POSITIONS, WIDTH)
    return (query_grad, key_grad, value_grad)
```

```python
import jax
import jax.numpy as jnp
from jax import lax
from jax.experimental import pallas as pl
from jax.experimental.pallas import tpu as pltpu
from jax.sharding import PartitionSpec as P

F32 = jnp.float32
BF16 = jnp.bfloat16
MESH = pl.DeviceIdType.MESH
AXES = ("gx", "gy", "gz")
HEADS = 4
DIM = 256
ROWS = 512
HALF = DIM // 2
CHUNKS = 2
SIDE = 4
CHIPS = SIDE**3
PEERS = sorted(
    (
        (dx, dy, dz)
        for dx in range(SIDE)
        for dy in range(SIDE)
        for dz in range(SIDE)
        if (dx, dy, dz) != (0, 0, 0)
    ),
    key=lambda o: -sum(min(d, SIDE - d) for d in o),
)


def dot(a, b, contract):
    return lax.dot_general(a, b, ((contract[:1], contract[1:]), ((), ())), preferred_element_type=F32)


def columns(h):
    return pl.ds(h * DIM, DIM)


def wait_bytes(ref, sem):
    pltpu.make_async_copy(ref, ref, sem).wait()


def cumulative_rows(ld):
    high = ld.astype(BF16)
    rest = ld - high.astype(F32)
    middle = rest.astype(BF16)
    low = (rest - middle.astype(F32)).astype(BF16)
    upto = lax.broadcasted_iota(jnp.int32, (ROWS, ROWS), 0) <= lax.broadcasted_iota(
        jnp.int32, (ROWS, ROWS), 1
    )
    ones = jnp.where(upto, 1.0, 0.0).astype(BF16)
    return (
        dot(high, ones, (1, 0)) + dot(middle, ones, (1, 0)) + dot(low, ones, (1, 0))
    )


def exchange_kernel(
    q_hbm, k_hbm, v_hbm, g_hbm, ld_hbm, st_hbm,
    qg, kp, vp, gi, te,
    q, k, v, g, ld, st,
    brow, bcol, start, local, other, total, arrived, carried, carry, pair_out, pair_in,
    own_decay, pair_decay, chip_decay, all_decay,
    in_sems, pair_sems, there_sems, back_sems, home_sems, decay_sems,
):
    gx, gy, gz = (lax.axis_index(a) for a in AXES)
    z, core = gz // 2, gz % 2
    me = (gx * SIDE + gy) * SIDE + z
    partner = (gx, gy, z * 2 + (1 - core))
    scale = DIM**-0.5

    def peer(o):
        x, y, w = (gx + o[0]) % SIDE, (gy + o[1]) % SIDE, (z + o[2]) % SIDE
        return (x, y, w * 2 + core), (x * SIDE + y) * SIDE + w, x // (SIDE // 2)

    loads = [
        pltpu.make_async_copy(a, b, in_sems.at[i])
        for i, (a, b) in enumerate(
            ((ld_hbm, ld), (q_hbm, q), (g_hbm, g), (k_hbm, k), (v_hbm, v), (st_hbm, st))
        )
    ]
    for copy in loads:
        copy.start()
    barrier = pltpu.get_barrier_semaphore()
    for o in PEERS:
        pl.semaphore_signal(barrier, inc=1, device_id=peer(o)[0], device_id_type=MESH)
    pl.semaphore_signal(barrier, inc=1, device_id=partner, device_id_type=MESH)

    loads[0].wait()
    b = cumulative_rows(jnp.concatenate([ld[...], jnp.zeros_like(ld)], axis=0))
    end = b[:, ROWS - 1 :]
    brow[...] = b
    bcol[...] = b.T
    start[...] = (scale * jnp.exp(b)).T
    te[...] = jnp.exp(end - b).T
    own_decay[...] = jnp.broadcast_to(jnp.exp(end), (8, 128))

    loads[1].wait()
    loads[2].wait()
    for h in range(HEADS):
        decayed = (q[:, columns(h)].astype(F32) * start[:, h : h + 1]).astype(BF16)
        gh = g[:, columns(h)]
        for half in range(2):
            local[h, half] = dot(decayed[:, half * HALF : (half + 1) * HALF], gh, (0, 0))

    pl.semaphore_wait(barrier, len(PEERS) + 1)

    swap_decay = pltpu.make_async_remote_copy(
        src_ref=own_decay, dst_ref=pair_decay, send_sem=decay_sems.at[0], recv_sem=decay_sems.at[1],
        device_id=partner, device_id_type=MESH,
    )
    swap_decay.start()
    swaps = []
    for ch in range(CHUNKS):
        for i in range(2):
            h = ch * 2 + i
            swaps.append(
                pltpu.make_async_remote_copy(
                    src_ref=local.at[h, 1 - core], dst_ref=other.at[h],
                    send_sem=pair_sems.at[0, h], recv_sem=pair_sems.at[1, h],
                    device_id=partner, device_id_type=MESH,
                )
            )
            swaps[-1].start()

    first = core == 0
    swap_decay.wait_recv()
    mine, theirs = own_decay[...], pair_decay[...]
    product = mine * theirs
    for i in range(2):
        chip_decay[i] = jnp.concatenate([product[i : i + 1], product[2 + i : 3 + i]], axis=0)
    all_decay[me] = chip_decay[gx // (SIDE // 2)]
    own_factor = jnp.where(first, 1.0, theirs)
    pair_factor = jnp.where(first, mine, 1.0)

    def send_all(source, target, by_sender, sems):
        for o in PEERS:
            device, theirs_at, _ = peer(o)
            pltpu.make_async_remote_copy(
                src_ref=source.at[theirs_at], dst_ref=target.at[me],
                send_sem=sems.at[0], recv_sem=sems.at[1],
                device_id=device, device_id_type=MESH,
            ).start()

    def wait_sent(ref, sems):
        wait_bytes(ref.at[pl.ds(0, CHIPS - 1)], sems.at[0])

    def wait_arrived(ref, sems):
        wait_bytes(ref.at[pl.ds(0, CHIPS - 1)], sems.at[1])

    for o in PEERS:
        device, _, half = peer(o)
        pltpu.make_async_remote_copy(
            src_ref=chip_decay.at[half], dst_ref=all_decay.at[me],
            send_sem=decay_sems.at[2], recv_sem=decay_sems.at[3],
            device_id=device, device_id_type=MESH,
        ).start()

    for ch in range(CHUNKS):
        for i in range(2):
            h = ch * 2 + i
            swaps[h].wait_recv()
            chip = local[h, core] * own_factor[h : h + 1, :1] + other[h] * pair_factor[h : h + 1, :1]
            for j in range(2):
                total[ch, pl.ds(i * 32 + j * 16, 16)] = chip[:, j * 128 : (j + 1) * 128].reshape(
                    16, 8, 128
                )
        send_all(total.at[ch], arrived.at[ch], None, there_sems.at[ch])
        arrived[ch, me] = total[ch, me]

    loads[3].wait()
    loads[4].wait()
    loads[5].wait()

    def inside(h):
        blocks = [[None, None], [None, None]]
        for s in range(2):
            for t in range(s, 2):
                at_s, at_t = pl.ds(s * 256, 256), pl.ds(t * 256, 256)
                gap = brow[h : h + 1, t * 256 : (t + 1) * 256] - bcol[at_s, h : h + 1]
                weight = jnp.exp(jnp.minimum(gap, 0.0)) * scale
                if s == t:
                    keep = lax.broadcasted_iota(jnp.int32, (256, 256), 0) <= lax.broadcasted_iota(
                        jnp.int32, (256, 256), 1
                    )
                    weight = jnp.where(keep, weight, 0.0)
                probs = (dot(k[at_s, columns(h)], q[at_t, columns(h)], (1, 1)) * weight).astype(BF16)
                grads = (dot(v[at_s, columns(h)], g[at_t, columns(h)], (1, 1)) * weight).astype(BF16)
                blocks[s][t] = (probs, grads)
        for s in range(2):
            at_s = pl.ds(s * 256, 256)
            kp[at_s, columns(h)] = sum(
                dot(blocks[s][t][1], q[pl.ds(t * 256, 256), columns(h)], (1, 0)) for t in range(s, 2)
            )
            vp[at_s, columns(h)] = sum(
                dot(blocks[s][t][0], g[pl.ds(t * 256, 256), columns(h)], (1, 0)) for t in range(s, 2)
            )
        for t in range(2):
            at_t = pl.ds(t * 256, 256)
            inner = sum(
                dot(blocks[s][t][1], k[pl.ds(s * 256, 256), columns(h)], (0, 0)) for s in range(t + 1)
            )
            from_state = dot(g[at_t, columns(h)], st[0, h], (1, 1)) * start[at_t, h : h + 1]
            qg[at_t, columns(h)] = (inner + from_state).astype(BF16)

    inside(0)
    inside(1)

    wait_arrived(all_decay, decay_sems.at[pl.ds(2, 2)])
    for ch in range(CHUNKS):
        wait_arrived(arrived.at[ch], there_sems.at[ch])
        running = jnp.zeros((8, 128), F32)
        for m in reversed(range(CHIPS)):
            carried[ch, m] = running
            running = running * all_decay[m, ch : ch + 1] + arrived[ch, m]
        send_all(carried.at[ch], carry.at[ch], None, back_sems.at[ch])
        carry[ch, me] = carried[ch, me]

    inside(2)
    inside(3)

    own_a, own_b = jnp.where(first, theirs, 1.0), jnp.where(first, 1.0, 0.0)
    out_a, out_b = jnp.where(first, 1.0, mine), jnp.where(first, 0.0, 1.0)
    homes = []
    for ch in range(CHUNKS):
        wait_arrived(carry.at[ch], back_sems.at[ch])
        for i in range(2):
            h = ch * 2 + i
            later = jnp.concatenate(
                [carry[ch, pl.ds(i * 32 + j * 16, 16)].reshape(128, 128) for j in range(2)], axis=1
            )
            pair_out[h] = later * out_a[h : h + 1, :1] + local[h, core] * out_b
            homes.append(
                pltpu.make_async_remote_copy(
                    src_ref=pair_out.at[h], dst_ref=pair_in.at[h],
                    send_sem=home_sems.at[0, h], recv_sem=home_sems.at[1, h],
                    device_id=partner, device_id_type=MESH,
                )
            )
            homes[-1].start()
            gi[h, core] = (later * own_a[h : h + 1, :1] + other[h] * own_b).astype(BF16)
    for h in range(HEADS):
        homes[h].wait_recv()
        gi[h, 1 - core] = pair_in[h].astype(BF16)

    swap_decay.wait_send()
    for copy in swaps + homes:
        copy.wait_send()
    wait_sent(all_decay, decay_sems.at[pl.ds(2, 2)])
    for ch in range(CHUNKS):
        wait_sent(total.at[ch], there_sems.at[ch])
        wait_sent(carried.at[ch], back_sems.at[ch])


def finish_kernel(k, v, qg_in, kp, vp, gi, te, qg, kg, vg):
    qg[...] = qg_in[...]
    h = pl.program_id(0)
    lane = lax.broadcasted_iota(jnp.int32, (ROWS, 8), 1)
    end = jnp.sum(jnp.where(lane == h, te[...], 0.0), axis=1, keepdims=True)
    grad_in = gi[0]
    kg[...] = (kp[...] + dot(v[...], grad_in, (1, 1)) * end).astype(BF16)
    vg[...] = (vp[...] + dot(k[...], grad_in, (1, 0)) * end).astype(BF16)


def body(queries, keys, values, out_grad, log_decay, saved_states):
    wide = (ROWS, HEADS * DIM)
    anywhere = pl.BlockSpec(memory_space=pltpu.HBM)
    vmem = pl.BlockSpec(memory_space=pltpu.VMEM)
    dma = pltpu.SemaphoreType.DMA
    pieces = pltpu.VMEM((CHUNKS, CHIPS, 8, 128), F32)
    halves = pltpu.VMEM((HEADS, HALF, DIM), F32)
    qg, kp, vp, gi, te = pl.pallas_call(
        exchange_kernel,
        out_shape=(
            jax.ShapeDtypeStruct(wide, BF16),
            jax.ShapeDtypeStruct(wide, F32),
            jax.ShapeDtypeStruct(wide, F32),
            jax.ShapeDtypeStruct((HEADS, 2, HALF, DIM), BF16),
            jax.ShapeDtypeStruct((ROWS, 8), F32),
        ),
        in_specs=[anywhere] * 6,
        out_specs=(vmem,) * 5,
        scratch_shapes=[
            pltpu.VMEM(wide, BF16), pltpu.VMEM(wide, BF16), pltpu.VMEM(wide, BF16), pltpu.VMEM(wide, BF16),
            pltpu.VMEM((HEADS, ROWS), F32), pltpu.VMEM((1, HEADS, DIM, DIM), BF16),
            pltpu.VMEM((8, ROWS), F32), pltpu.VMEM((ROWS, 8), F32), pltpu.VMEM((ROWS, 8), F32),
            pltpu.VMEM((HEADS, 2, HALF, DIM), F32), halves,
            pieces, pieces, pieces, pieces, halves, halves,
            pltpu.VMEM((8, 128), F32), pltpu.VMEM((8, 128), F32),
            pltpu.VMEM((2, CHUNKS, 128), F32), pltpu.VMEM((CHIPS, CHUNKS, 128), F32),
            dma((6,)), dma((2, HEADS)), dma((CHUNKS, 2)), dma((CHUNKS, 2)), dma((2, HEADS)), dma((4,)),
        ],
        compiler_params=pltpu.CompilerParams(
            collective_id=0, has_side_effects=True, vmem_limit_bytes=32 << 20
        ),
        cost_estimate=pl.CostEstimate(flops=4_000_000_000, bytes_accessed=8 << 20, transcendentals=0),
        name="exchange",
    )(queries, keys, values, out_grad, log_decay, saved_states)
    gi = gi.reshape(HEADS, DIM, DIM)
    by_head = pl.BlockSpec((ROWS, DIM), lambda h: (0, h))
    return pl.pallas_call(
        finish_kernel,
        grid=(HEADS,),
        out_shape=(jax.ShapeDtypeStruct(wide, BF16),) * 3,
        in_specs=[
            by_head, by_head, by_head, by_head, by_head,
            pl.BlockSpec((1, DIM, DIM), lambda h: (h, 0, 0)),
            pl.BlockSpec((ROWS, 8), lambda h: (0, 0)),
        ],
        out_specs=(by_head,) * 3,
        compiler_params=pltpu.CompilerParams(vmem_limit_bytes=16 << 20),
        cost_estimate=pl.CostEstimate(flops=600_000_000, bytes_accessed=8 << 20, transcendentals=0),
        name="finish",
    )(keys, values, qg, kp, vp, gi, te)


def solution(mesh):
    rows = P(AXES, None)
    return jax.shard_map(
        body,
        mesh=mesh,
        in_specs=(rows, rows, rows, rows, P(None, AXES), P(AXES, None, None, None)),
        out_specs=(rows, rows, rows),
        check_vma=False,
    )
```

```python
import jax
import jax.numpy as jnp
from jax import lax
from jax.experimental import pallas as pl
from jax.experimental.pallas import tpu as pltpu
from jax.sharding import PartitionSpec as P

F32 = jnp.float32
BF16 = jnp.bfloat16
MESH = pl.DeviceIdType.MESH
AXES = ("gx", "gy", "gz")
HEADS = 4
DIM = 256
ROWS = 512
HALF = DIM // 2
CHUNKS = 2
SIDE = 4
CHIPS = SIDE**3
PEERS = sorted(
    (
        (dx, dy, dz)
        for dx in range(SIDE)
        for dy in range(SIDE)
        for dz in range(SIDE)
        if (dx, dy, dz) != (0, 0, 0)
    ),
    key=lambda o: -sum(min(d, SIDE - d) for d in o),
)


def dot(a, b, contract):
    return lax.dot_general(a, b, ((contract[:1], contract[1:]), ((), ())), preferred_element_type=F32)


def columns(h):
    return pl.ds(h * DIM, DIM)


def wait_bytes(ref, sem):
    pltpu.make_async_copy(ref, ref, sem).wait()


def cumulative_rows(ld):
    high = ld.astype(BF16)
    rest = ld - high.astype(F32)
    middle = rest.astype(BF16)
    low = (rest - middle.astype(F32)).astype(BF16)
    upto = lax.broadcasted_iota(jnp.int32, (ROWS, ROWS), 0) <= lax.broadcasted_iota(
        jnp.int32, (ROWS, ROWS), 1
    )
    ones = jnp.where(upto, 1.0, 0.0).astype(BF16)
    return (
        dot(high, ones, (1, 0)) + dot(middle, ones, (1, 0)) + dot(low, ones, (1, 0))
    )


def exchange_kernel(
    q_hbm, k_hbm, v_hbm, g_hbm, ld_hbm, st_hbm,
    qg, kg, vg,
    q, k, v, g, ld, st, kp, vp, gi, te,
    brow, bcol, start, local, other, total, arrived, carried, carry, pair_out, pair_in,
    own_decay, pair_decay, chip_decay, all_decay,
    in_sems, pair_sems, there_sems, back_sems, home_sems, decay_sems,
):
    gx, gy, gz = (lax.axis_index(a) for a in AXES)
    z, core = gz // 2, gz % 2
    me = (gx * SIDE + gy) * SIDE + z
    partner = (gx, gy, z * 2 + (1 - core))
    scale = DIM**-0.5

    def peer(o):
        x, y, w = (gx + o[0]) % SIDE, (gy + o[1]) % SIDE, (z + o[2]) % SIDE
        return (x, y, w * 2 + core), (x * SIDE + y) * SIDE + w, x // (SIDE // 2)

    loads = [
        pltpu.make_async_copy(a, b, in_sems.at[i])
        for i, (a, b) in enumerate(
            ((ld_hbm, ld), (q_hbm, q), (g_hbm, g), (k_hbm, k), (v_hbm, v), (st_hbm, st))
        )
    ]
    for copy in loads:
        copy.start()
    barrier = pltpu.get_barrier_semaphore()
    for o in PEERS:
        pl.semaphore_signal(barrier, inc=1, device_id=peer(o)[0], device_id_type=MESH)
    pl.semaphore_signal(barrier, inc=1, device_id=partner, device_id_type=MESH)

    loads[0].wait()
    b = cumulative_rows(jnp.concatenate([ld[...], jnp.zeros_like(ld)], axis=0))
    end = b[:, ROWS - 1 :]
    brow[...] = b
    bcol[...] = b.T
    start[...] = (scale * jnp.exp(b)).T
    te[...] = jnp.exp(end - b).T
    own_decay[...] = jnp.broadcast_to(jnp.exp(end), (8, 128))

    loads[1].wait()
    loads[2].wait()
    for h in range(HEADS):
        decayed = (q[:, columns(h)].astype(F32) * start[:, h : h + 1]).astype(BF16)
        gh = g[:, columns(h)]
        for half in range(2):
            local[h, half] = dot(decayed[:, half * HALF : (half + 1) * HALF], gh, (0, 0))

    pl.semaphore_wait(barrier, len(PEERS) + 1)

    swap_decay = pltpu.make_async_remote_copy(
        src_ref=own_decay, dst_ref=pair_decay, send_sem=decay_sems.at[0], recv_sem=decay_sems.at[1],
        device_id=partner, device_id_type=MESH,
    )
    swap_decay.start()
    swaps = []
    for ch in range(CHUNKS):
        for i in range(2):
            h = ch * 2 + i
            swaps.append(
                pltpu.make_async_remote_copy(
                    src_ref=local.at[h, 1 - core], dst_ref=other.at[h],
                    send_sem=pair_sems.at[0, h], recv_sem=pair_sems.at[1, h],
                    device_id=partner, device_id_type=MESH,
                )
            )
            swaps[-1].start()

    first = core == 0
    swap_decay.wait_recv()
    mine, theirs = own_decay[...], pair_decay[...]
    product = mine * theirs
    for i in range(2):
        chip_decay[i] = jnp.concatenate([product[i : i + 1], product[2 + i : 3 + i]], axis=0)
    all_decay[me] = chip_decay[gx // (SIDE // 2)]
    own_factor = jnp.where(first, 1.0, theirs)
    pair_factor = jnp.where(first, mine, 1.0)

    def send_all(source, target, by_sender, sems):
        for o in PEERS:
            device, theirs_at, _ = peer(o)
            pltpu.make_async_remote_copy(
                src_ref=source.at[theirs_at], dst_ref=target.at[me],
                send_sem=sems.at[0], recv_sem=sems.at[1],
                device_id=device, device_id_type=MESH,
            ).start()

    def wait_sent(ref, sems):
        wait_bytes(ref.at[pl.ds(0, CHIPS - 1)], sems.at[0])

    def wait_arrived(ref, sems):
        wait_bytes(ref.at[pl.ds(0, CHIPS - 1)], sems.at[1])

    for o in PEERS:
        device, _, half = peer(o)
        pltpu.make_async_remote_copy(
            src_ref=chip_decay.at[half], dst_ref=all_decay.at[me],
            send_sem=decay_sems.at[2], recv_sem=decay_sems.at[3],
            device_id=device, device_id_type=MESH,
        ).start()

    for ch in range(CHUNKS):
        for i in range(2):
            h = ch * 2 + i
            swaps[h].wait_recv()
            chip = local[h, core] * own_factor[h : h + 1, :1] + other[h] * pair_factor[h : h + 1, :1]
            for j in range(2):
                total[ch, pl.ds(i * 32 + j * 16, 16)] = chip[:, j * 128 : (j + 1) * 128].reshape(
                    16, 8, 128
                )
        send_all(total.at[ch], arrived.at[ch], None, there_sems.at[ch])
        arrived[ch, me] = total[ch, me]

    loads[3].wait()
    loads[4].wait()
    loads[5].wait()

    def inside(h):
        blocks = [[None, None], [None, None]]
        for s in range(2):
            for t in range(s, 2):
                at_s, at_t = pl.ds(s * 256, 256), pl.ds(t * 256, 256)
                gap = brow[h : h + 1, t * 256 : (t + 1) * 256] - bcol[at_s, h : h + 1]
                weight = jnp.exp(jnp.minimum(gap, 0.0)) * scale
                if s == t:
                    keep = lax.broadcasted_iota(jnp.int32, (256, 256), 0) <= lax.broadcasted_iota(
                        jnp.int32, (256, 256), 1
                    )
                    weight = jnp.where(keep, weight, 0.0)
                probs = (dot(k[at_s, columns(h)], q[at_t, columns(h)], (1, 1)) * weight).astype(BF16)
                grads = (dot(v[at_s, columns(h)], g[at_t, columns(h)], (1, 1)) * weight).astype(BF16)
                blocks[s][t] = (probs, grads)
        for s in range(2):
            at_s = pl.ds(s * 256, 256)
            kp[at_s, columns(h)] = sum(
                dot(blocks[s][t][1], q[pl.ds(t * 256, 256), columns(h)], (1, 0)) for t in range(s, 2)
            )
            vp[at_s, columns(h)] = sum(
                dot(blocks[s][t][0], g[pl.ds(t * 256, 256), columns(h)], (1, 0)) for t in range(s, 2)
            )
        for t in range(2):
            at_t = pl.ds(t * 256, 256)
            inner = sum(
                dot(blocks[s][t][1], k[pl.ds(s * 256, 256), columns(h)], (0, 0)) for s in range(t + 1)
            )
            from_state = dot(g[at_t, columns(h)], st[0, h], (1, 1)) * start[at_t, h : h + 1]
            qg[at_t, columns(h)] = (inner + from_state).astype(BF16)

    inside(0)
    inside(1)

    wait_arrived(all_decay, decay_sems.at[pl.ds(2, 2)])
    for ch in range(CHUNKS):
        wait_arrived(arrived.at[ch], there_sems.at[ch])
        running = jnp.zeros((8, 128), F32)
        for m in reversed(range(CHIPS)):
            carried[ch, m] = running
            running = running * all_decay[m, ch : ch + 1] + arrived[ch, m]
        send_all(carried.at[ch], carry.at[ch], None, back_sems.at[ch])
        carry[ch, me] = carried[ch, me]

    inside(2)
    inside(3)

    own_a, own_b = jnp.where(first, theirs, 1.0), jnp.where(first, 1.0, 0.0)
    out_a, out_b = jnp.where(first, 1.0, mine), jnp.where(first, 0.0, 1.0)
    homes = []
    for ch in range(CHUNKS):
        wait_arrived(carry.at[ch], back_sems.at[ch])
        for i in range(2):
            h = ch * 2 + i
            later = jnp.concatenate(
                [carry[ch, pl.ds(i * 32 + j * 16, 16)].reshape(128, 128) for j in range(2)], axis=1
            )
            pair_out[h] = later * out_a[h : h + 1, :1] + local[h, core] * out_b
            homes.append(
                pltpu.make_async_remote_copy(
                    src_ref=pair_out.at[h], dst_ref=pair_in.at[h],
                    send_sem=home_sems.at[0, h], recv_sem=home_sems.at[1, h],
                    device_id=partner, device_id_type=MESH,
                )
            )
            homes[-1].start()
            gi[h, core] = (later * own_a[h : h + 1, :1] + other[h] * own_b).astype(BF16)
    for h in range(HEADS):
        homes[h].wait_recv()
        gi[h, 1 - core] = pair_in[h].astype(BF16)
        grad_in, to_end = gi[h].reshape(DIM, DIM), te[:, h : h + 1]
        kg[:, columns(h)] = (kp[:, columns(h)] + dot(v[:, columns(h)], grad_in, (1, 1)) * to_end).astype(BF16)
        vg[:, columns(h)] = (vp[:, columns(h)] + dot(k[:, columns(h)], grad_in, (1, 0)) * to_end).astype(BF16)

    swap_decay.wait_send()
    for copy in swaps + homes:
        copy.wait_send()
    wait_sent(all_decay, decay_sems.at[pl.ds(2, 2)])
    for ch in range(CHUNKS):
        wait_sent(total.at[ch], there_sems.at[ch])
        wait_sent(carried.at[ch], back_sems.at[ch])


def write_kernel(*refs):
    count = len(refs) // 2
    copies = [
        pltpu.make_async_copy(source, target, refs[-1].at[i])
        for i, (source, target) in enumerate(zip(refs[:count], refs[count:-1]))
    ]
    for copy in copies:
        copy.start()
    for copy in copies:
        copy.wait()


def body(*arrays):
    wide = jax.ShapeDtypeStruct((ROWS, HEADS * DIM), BF16)
    dma = pltpu.SemaphoreType.DMA
    hbm, vmem = (pl.BlockSpec(memory_space=space) for space in (pltpu.HBM, pltpu.VMEM))
    rows = pltpu.VMEM(wide.shape, BF16)
    sums = pltpu.VMEM(wide.shape, F32)
    pieces = pltpu.VMEM((CHUNKS, CHIPS, 8, 128), F32)
    halves = pltpu.VMEM((HEADS, HALF, DIM), F32)
    grads = pl.pallas_call(
        exchange_kernel,
        out_shape=(wide,) * 3,
        in_specs=[hbm] * 6,
        out_specs=(vmem,) * 3,
        scratch_shapes=[
            rows, rows, rows, rows,
            pltpu.VMEM((HEADS, ROWS), F32), pltpu.VMEM((1, HEADS, DIM, DIM), BF16),
            sums, sums, pltpu.VMEM((HEADS, 2, HALF, DIM), BF16), pltpu.VMEM((ROWS, 8), F32),
            pltpu.VMEM((8, ROWS), F32), pltpu.VMEM((ROWS, 8), F32), pltpu.VMEM((ROWS, 8), F32),
            pltpu.VMEM((HEADS, 2, HALF, DIM), F32), halves,
            pieces, pieces, pieces, pieces, halves, halves,
            pltpu.VMEM((8, 128), F32), pltpu.VMEM((8, 128), F32),
            pltpu.VMEM((2, CHUNKS, 128), F32), pltpu.VMEM((CHIPS, CHUNKS, 128), F32),
            dma((6,)), dma((2, HEADS)), dma((CHUNKS, 2)), dma((CHUNKS, 2)), dma((2, HEADS)), dma((4,)),
        ],
        compiler_params=pltpu.CompilerParams(
            collective_id=0, has_side_effects=True, vmem_limit_bytes=40 << 20
        ),
        cost_estimate=pl.CostEstimate(flops=4_000_000_000, bytes_accessed=8 << 20, transcendentals=0),
        name="exchange",
    )(*(pltpu.with_memory_space_constraint(x, pltpu.HBM) for x in arrays))
    return pl.pallas_call(
        write_kernel,
        out_shape=(wide,) * 3,
        in_specs=[vmem] * 3,
        out_specs=(hbm,) * 3,
        scratch_shapes=[dma((3,))],
        compiler_params=pltpu.CompilerParams(vmem_limit_bytes=8 << 20),
        name="write",
    )(*grads)


def solution(mesh):
    rows = P(AXES, None)
    return jax.shard_map(
        body,
        mesh=mesh,
        in_specs=(rows, rows, rows, rows, P(None, AXES), P(AXES, None, None, None)),
        out_specs=(rows, rows, rows),
        check_vma=False,
    )
```
